256 devices in a mesh: row: 16 (over z_lo, y), col: 16 (over z_hi, x, core).
Axes of the slice: x: 4, y: 4, z: 8 (z_hi: 2, z_lo: 4; z = z_hi * 4 + z_lo), core: 2. Of those that a mesh axis runs over, the one named last changes fastest.
Arguments:
- orbitals: float32 [2048, 28672], P(('row', 'col')), may hold values from -0.03125 to 0.03125
- applied: float32 [2048, 28672], P(('row', 'col')), may hold values from -24 to 24
Outputs:
- hamiltonian: float32 [2048, 2048], P('col', 'row')
- intersection: float32 [2048, 2048], P('col', 'row')
The draws below stay inside these ranges and needn't reach their ends.
All inputs are finite; a program needn't handle non-finite values.
Results may differ from the reference program's by a relative error of at most 0.000098.
Values sent between devices are 32-bit elements; how exact they have to be, the bound alone decides.
No kernel may reach another device: no remote copies, remote signals or barrier semaphores. Data moves between devices by JAX's collectives and lax.ppermute only.
A program may use at most 64 MiB of HBM per device.

```python
import jax
import jax.numpy as jnp
from jax import lax

NORB = 2048
NCOEF = 28672


def strengthened(values, stream_key, source, target, shards_of, factor):
    def block_of(dim):
        return (jnp.arange(values.shape[dim]) // (values.shape[dim] // shards_of)).reshape((-1,) + (1,) * (values.ndim - 1 - dim))

    near = jax.random.permutation(stream_key, shards_of)[block_of(target)]
    other_side = (block_of(target) + shards_of // 2) % shards_of
    return jnp.where((block_of(source) == near) | (block_of(source) == other_side), factor * values, values)


def block_scale(rng, extent, pieces, smallest, largest):
    gain, own = 1.0, jax.random.fold_in(rng, 6)
    for position, parts in pieces:
        steps = jnp.exp(jax.random.uniform(jax.random.fold_in(own, position), (parts,), jnp.float32, smallest / len(pieces), largest / len(pieces)))
        gain = gain * jnp.repeat(steps, extent[position] // parts).reshape([-1 if axis == position else 1 for axis in range(len(extent))])
    return gain


def noise(key, dims, spread, bound, split=(), dtype=jnp.bfloat16):
    level = block_scale(key, dims, split, -0.22, 0.18) if split else 1.0
    values = jax.random.normal(key, dims, jnp.float32) * spread * level
    return jnp.minimum(jnp.maximum(values, -bound), bound).astype(dtype)


def noise_with(stream_key, extent, deviation, most, pieces, heavy, dtype=jnp.bfloat16):
    drawn = deviation * jax.random.normal(stream_key, extent, jnp.float32)
    if pieces:
        drawn = drawn * block_scale(stream_key, extent, pieces, -0.22, 0.18)
    return jnp.clip(strengthened(drawn, jax.random.fold_in(stream_key, 3), *heavy), -most, most).astype(dtype)


def setup_inputs(seed: int = 0) -> dict:
    key_of = jax.random.split(jax.random.key(seed), 3)
    return {
        "orbitals": noise(key_of[0], (NORB, NCOEF), NCOEF ** -0.5, 0.03125, ((0, 256),), jnp.float32),
        "applied": noise_with(key_of[1], (NORB, NCOEF), 1.0, 24.0, ((0, 256),), (1, 0, 256, 6.0), jnp.float32),
    }


def reference(orbitals, applied):
    hamiltonian = jnp.dot(orbitals, applied.T, precision=lax.Precision.HIGHEST, preferred_element_type=jnp.float32)
    intersection = jnp.dot(orbitals, orbitals.T, precision=lax.Precision.HIGHEST, preferred_element_type=jnp.float32)
    return hamiltonian, intersection
```

```python
import jax
import jax.numpy as jnp
from jax import lax
from jax.sharding import Mesh, PartitionSpec as P

AXES = ("zlo", "y", "zhi", "x", "core")
Z = ("zlo", "zhi")
CHUNKS = 2


def z_ring(step):
    place = lambda z: (z % 4) * 2 + z // 4
    return [(place(z), place((z + step) % 8)) for z in range(8)]


def product(left, right):
    return lax.dot_general(
        left,
        right,
        (((1,), (1,)), ((), ())),
        precision=lax.Precision.HIGH,
        preferred_element_type=jnp.float32,
    )


def both_cores(mine, core):
    other = lax.ppermute(mine, "core", [(0, 1), (1, 0)])
    k = mine.shape[-1]
    mine, other = mine.reshape(4, 4, 1, 8, k), other.reshape(4, 4, 1, 8, k)
    first = core == 0
    return jnp.concatenate([jnp.where(first, mine, other), jnp.where(first, other, mine)], 2)


def body(orbitals, applied):
    core = lax.axis_index("core")
    z = lax.axis_index("zhi") * 4 + lax.axis_index("zlo")
    width = orbitals.shape[1] // CHUNKS

    def spread(a, c):
        piece = lax.slice_in_dim(a, c * width, (c + 1) * width, axis=1)
        return lax.all_to_all(piece, ("y", "x"), split_axis=1, concat_axis=0, tiled=True)

    orb = [both_cores(spread(orbitals, c), core) for c in range(CHUNKS)]
    k = width // 16
    blocks = []
    for o in orb:
        half = lax.dynamic_index_in_dim(o.reshape(2, 2, 64, k), core, axis=1, keepdims=False)
        blocks.append(half.reshape(128, k))
    app = [both_cores(spread(applied, c), core) for c in range(CHUNKS)]
    own = [
        jnp.stack([a.reshape(4, 64, k), o.reshape(4, 64, k)], 1).reshape(512, k)
        for a, o in zip(app, orb)
    ]

    held = {(0, c): blocks[c] for c in range(CHUNKS)}
    for d in range(1, 5):
        for c in range(CHUNKS):
            if d < 4 or c == 0:
                held[(d, c)] = lax.ppermute(held[(d - 1, c)], Z, z_ring(-1))
            if d < 4 or c == 1:
                got = lax.ppermute(held[((1 - d) % 8, c)], Z, z_ring(1))
                held[(-d % 8, c)] = got
    parts = []
    for d in range(8):
        parts.append(sum(product(held[(d, c)], own[c]) for c in range(CHUNKS)))
    part = jnp.stack(parts).reshape(8, 128, 4, 128)

    part = jnp.transpose(part, (2, 0, 1, 3))
    got = lax.all_to_all(part, "y", split_axis=0, concat_axis=0, tiled=True)
    part = got.sum(0)
    part = jnp.roll(part, z, axis=0)
    part = part.reshape(2, 2, 2, 2, 64, 128)
    part = jnp.transpose(part, (1, 2, 3, 0, 4, 5)).reshape(8, 2, 64, 128)
    got = lax.all_to_all(part, ("zhi", "x"), split_axis=0, concat_axis=0, tiled=True)
    tile = got.reshape(2, 4, 2, 64, 2, 64).sum(1)
    tile = jnp.transpose(tile, (3, 1, 2, 0, 4)).reshape(2, 128, 128)
    return tile[0], tile[1]


def solution(mesh):
    fine = Mesh(mesh.devices.reshape(4, 4, 2, 4, 2), AXES)
    placed = P(AXES, None)
    out = P(("zhi", "x", "core"), ("zlo", "y"))
    return jax.shard_map(
        body, mesh=fine, in_specs=(placed, placed), out_specs=(out, out), check_vma=False
    )
```

```python
import jax
import jax.numpy as jnp
from jax import lax
from jax.experimental import pallas as pl
from jax.experimental.pallas import tpu as pltpu
from jax.sharding import Mesh, PartitionSpec as P


AXES = ("zlo", "y", "zhi", "x", "core")
Z = ("zlo", "zhi")
F32, BF16 = jnp.float32, jnp.bfloat16
K = 1792
NT = (((1,), (1,)), ((), ()))
VMEM = pl.BlockSpec(memory_space=pltpu.VMEM)


def z_ring(step):
    place = lambda z: (z % 4) * 2 + z // 4
    return [(place(z), place((z + step) % 8)) for z in range(8)]


def ring(n, step):
    return [(i, (i + step) % n) for i in range(n)]


def call(kernel, shapes, *args, scratch=()):
    out = [jax.ShapeDtypeStruct(s, t) for s, t in shapes]
    return pl.pallas_call(
        kernel,
        out_shape=out,
        in_specs=[VMEM] * len(args),
        out_specs=[VMEM] * len(out),
        scratch_shapes=list(scratch),
        compiler_params=pltpu.CompilerParams(vmem_limit_bytes=20 * 2**20),
    )(*args)


def own_kernel(orb, same, cross, app, app_other, hi, lo):
    y, core = lax.axis_index("y"), lax.axis_index("core")
    first = core == 0

    def step(t, carry):
        ahead, x = t // 4, lax.rem(t, 4)
        to = lax.rem(y + ahead, 4)
        src = pl.ds(pl.multiple_of(to * 32 + x * 8, 8), 8)
        part = pl.ds(pl.multiple_of((to // 2) * 32 + x * 8, 8), 8)
        theirs = jnp.where(lax.rem(to, 2) == core, same[part, :], cross[part, :])
        for h, (a, b) in enumerate(((app[src, :], app_other[src, :]), (orb[src, :], theirs))):
            v = jnp.concatenate([jnp.where(first, a, b), jnp.where(first, b, a)], 0)
            top = v.astype(BF16)
            dst = pl.ds(pl.multiple_of(ahead * 128 + h * 64 + x * 16, 16), 16)
            hi[dst, :] = top
            lo[dst, :] = (v - top.astype(F32)).astype(BF16)
        return carry

    lax.fori_loop(0, 16, step, 0)


def product_kernel(n, hi, lo, *refs):
    blocks, outs = refs[: 2 * n], refs[2 * n :]
    v = jnp.concatenate([b[...] for b in blocks], 0)
    top = v.astype(BF16)
    low = (v - top.astype(F32)).astype(BF16)
    both = jnp.concatenate([top, low], 0)
    rows = n * 128
    for half in range(2):
        cols = slice(half * 256, (half + 1) * 256)
        p = lax.dot_general(both, hi[cols, :], NT, preferred_element_type=F32)
        r = lax.dot_general(top, lo[cols, :], NT, preferred_element_type=F32)
        total = (p[:rows] + p[rows:]) + r
        outs[2 * half][...] = total[:, :128]
        outs[2 * half + 1][...] = total[:, 128:]


def products(hi, lo, pairs):
    n = len(pairs)
    flat = [b for pair in pairs for b in pair]
    shapes = [((n * 128, 128), F32)] * 4
    return call(lambda *r: product_kernel(n, *r), shapes, hi, lo, *flat)


def to_y(parts):
    sent = [lax.ppermute(parts[q], "y", ring(4, q)) for q in range(1, 4)]
    return [parts[0]] + sent


def x_kernel(picks, refs, outs, sums):
    for m, (group, at) in enumerate(picks):
        rows = pl.ds(at * 128, 128)
        four = [r[rows, :] for r in refs[4 * group : 4 * group + 4]]
        sums[m] = (four[0] + four[1]) + (four[2] + four[3])
    x, zhi, zlo = lax.axis_index("x"), lax.axis_index("zhi"), lax.axis_index("zlo")
    for ahead in range(4):
        to = lax.rem(x + ahead, 4)
        xb, yh = to // 2, lax.rem(to, 2)
        for t in range(2):
            place = lax.rem(zhi + t, 2) * 2 + xb
            m = lax.rem(place - zlo + 4, 4)
            for h in range(2):
                at = t * 64 + h * 32
                outs[ahead][at : at + 32, :] = sums[
                    m, pl.ds(pl.multiple_of(h * 64 + yh * 32, 32), 32), :
                ]


def to_x(groups, picks):
    flat = [a for g in groups for a in g]
    n = len(flat)
    body = lambda *r: x_kernel(picks, r[:n], r[n : n + 4], r[n + 4])
    scratch = [pltpu.VMEM((4, 128, 128), F32)]
    outs = call(body, [((128, 128), F32)] * 4, *flat, scratch=scratch)
    got = [outs[0]] + [lax.ppermute(outs[q], "x", ring(4, q)) for q in range(1, 4)]

    def add(a, b, c, d, keep, send):
        v = (a[...] + b[...]) + (c[...] + d[...])
        keep[...] = v[:64]
        send[...] = v[64:]

    keep, send = call(add, [((64, 128), F32)] * 2, *got)
    return keep, lax.ppermute(send, "zhi", ring(2, 1))


def tile_kernel(keep_a, recv_a, keep_b, recv_b, ham, ovl):
    x, zhi, zlo = lax.axis_index("x"), lax.axis_index("zhi"), lax.axis_index("zlo")
    core = lax.axis_index("core")
    m = lax.rem(zhi * 2 + x // 2 - zlo + 4, 4)
    d = jnp.where(m < 2, m, m - 4)
    a0 = lax.rem(zhi * 4 + zlo + d + 8, 8) // 4
    for zi in range(2):
        parts = []
        for zj in range(2):
            far = lax.rem(zhi + zj, 2)
            late = lax.rem(zi + a0 + far, 2)
            kept = jnp.where(late == 0, keep_a[...], keep_b[...])
            came = jnp.where(late == 0, recv_a[...], recv_b[...])
            parts.append(jnp.where(far == 0, kept, came))
        for out, cut in ((ham, slice(0, 64)), (ovl, slice(64, 128))):
            v = jnp.concatenate([p[:, cut] for p in parts], axis=1)
            for h in range(2):
                c = lax.rem(core + h, 2)
                for k in range(4):
                    dst = pl.ds(pl.multiple_of(zi * 64 + k * 16 + c * 8, 8), 8)
                    out[dst, :] = v[h * 32 + k * 8 : h * 32 + k * 8 + 8, :]


def after(value, *others):
    return lax.optimization_barrier((value, *others))[0]


def body(orbitals, applied):
    core, swap = lax.axis_index("core"), ring(2, 1)
    orb = lax.all_to_all(orbitals, ("y", "x"), split_axis=1, concat_axis=0, tiled=True)
    by_parity = orb.reshape(2, 2, 32, K)
    mine = lax.dynamic_index_in_dim(by_parity, core, 1, False).reshape(64, K)
    theirs = lax.dynamic_index_in_dim(by_parity, 1 - core, 1, False).reshape(64, K)
    same = lax.ppermute(theirs, "core", swap)
    cross = lax.ppermute(mine, "core", swap)
    app = lax.all_to_all(after(applied, mine), ("y", "x"), split_axis=1, concat_axis=0, tiled=True)

    held = {(0, 0): mine, (0, 1): same}

    def forward(d, h):
        if d < 4 or h == 0:
            held[(d, h)] = lax.ppermute(held[(d - 1, h)], Z, z_ring(-1))
        if d < 4 or h == 1:
            held[(-d % 8, h)] = lax.ppermute(held[((1 - d) % 8, h)], Z, z_ring(1))

    for d in range(1, 5):
        for h in range(2):
            forward(d, h)
    app_other = lax.ppermute(app, "core", swap)
    hi, lo = call(own_kernel, [((512, K), BF16)] * 2, orb, same, cross, app, app_other)
    pair = lambda d: (held[(d % 8, 0)], held[(d % 8, 1)])
    y1 = to_y(products(hi, lo, [pair(0), pair(1), pair(-1)]))
    y2 = to_y(products(hi, lo, [pair(2), pair(-2)]))
    y3 = to_y(products(hi, lo, [pair(3), pair(-3)]))
    y4 = to_y(products(hi, lo, [pair(4)]))
    keep_a, recv_a = to_x([y1, y2], [(0, 0), (0, 1), (1, 1), (0, 2)])
    keep_b, recv_b = to_x([y2, y3, y4], [(2, 0), (1, 1), (0, 0), (1, 0)])
    return call(tile_kernel, [((128, 128), F32)] * 2, keep_a, recv_a, keep_b, recv_b)


def solution(mesh):
    fine = Mesh(mesh.devices.reshape(4, 4, 2, 4, 2), AXES)
    placed = P(AXES, None)
    out = P(("zhi", "x", "core"), ("zlo", "y"))

    return jax.shard_map(
        body, mesh=fine, in_specs=(placed, placed), out_specs=(out, out), check_vma=False
    )
```

```python
import jax
import jax.numpy as jnp
from jax import lax
from jax.experimental import pallas as pl
from jax.experimental.pallas import tpu as pltpu
from jax.sharding import Mesh, PartitionSpec as P


AXES = ("zlo", "y", "zhi", "x", "core")
Z = ("zlo", "zhi")
F32, BF16 = jnp.float32, jnp.bfloat16
K = 1792
NT = (((1,), (1,)), ((), ()))
VMEM = pl.BlockSpec(memory_space=pltpu.VMEM)


def z_ring(step):
    place = lambda z: (z % 4) * 2 + z // 4
    return [(place(z), place((z + step) % 8)) for z in range(8)]


def ring(n, step):
    return [(i, (i + step) % n) for i in range(n)]


def call(kernel, shapes, *args, scratch=()):
    out = [jax.ShapeDtypeStruct(s, t) for s, t in shapes]
    return pl.pallas_call(
        kernel,
        out_shape=out,
        in_specs=[VMEM] * len(args),
        out_specs=[VMEM] * len(out),
        scratch_shapes=list(scratch),
        compiler_params=pltpu.CompilerParams(vmem_limit_bytes=20 * 2**20),
    )(*args)


def own_kernel(orb, same, cross, app, app_other, hi, lo):
    y, core = lax.axis_index("y"), lax.axis_index("core")
    first = core == 0

    def step(t, carry):
        ahead, x = t // 4, lax.rem(t, 4)
        to = lax.rem(y + ahead, 4)
        src = pl.ds(pl.multiple_of(to * 32 + x * 8, 8), 8)
        part = pl.ds(pl.multiple_of((to // 2) * 32 + x * 8, 8), 8)
        theirs = jnp.where(lax.rem(to, 2) == core, same[part, :], cross[part, :])
        for h, (a, b) in enumerate(((app[src, :], app_other[src, :]), (orb[src, :], theirs))):
            v = jnp.concatenate([jnp.where(first, a, b), jnp.where(first, b, a)], 0)
            top = v.astype(BF16)
            dst = pl.ds(pl.multiple_of(ahead * 128 + h * 64 + x * 16, 16), 16)
            hi[dst, :] = top
            lo[dst, :] = (v - top.astype(F32)).astype(BF16)
        return carry

    lax.fori_loop(0, 16, step, 0)


def product(blocks, hi, lo):
    v = jnp.concatenate([b[...] for b in blocks], 0)
    top = v.astype(BF16)
    low = (v - top.astype(F32)).astype(BF16)
    both = jnp.concatenate([top, low], 0)
    rows, parts = v.shape[0], []
    for half in range(2):
        cols = slice(half * 256, (half + 1) * 256)
        p = lax.dot_general(both, hi[cols, :], NT, preferred_element_type=F32)
        r = lax.dot_general(top, lo[cols, :], NT, preferred_element_type=F32)
        total = (p[:rows] + p[rows:]) + r
        parts += [total[:, :128], total[:, 128:]]
    return parts


def products(hi, lo, blocks, groups=1):
    rows = sum(b.shape[0] for b in blocks) // groups

    def kernel(hi, lo, *refs):
        n = len(blocks)
        for q, part in enumerate(product(refs[:n], hi, lo)):
            for g in range(groups):
                refs[n + 4 * g + q][...] = part[g * rows : (g + 1) * rows]

    outs = call(kernel, [((rows, 128), F32)] * (4 * groups), hi, lo, *blocks)
    return [outs[4 * g : 4 * g + 4] for g in range(groups)]


def last_products(hi, lo, blocks, three):

    def kernel(hi, lo, *refs):
        n = len(blocks)
        out = refs[-1]
        y, zlo = lax.axis_index("y"), lax.axis_index("zlo")
        four = product(refs[:n], hi, lo)
        for d, parts in ((3, [r[...] for r in refs[n : n + 4]]), (4, four)):
            xb = lax.rem(zlo + d, 2)
            for q in range(4):
                to = lax.rem(y + q, 4) * 4 + xb * 2
                for yh in range(2):
                    for h in range(2):
                        at = pl.multiple_of((to + yh) * 64 + h * 32, 32)
                        src = h * 64 + yh * 32
                        out[pl.ds(at, 32), :] = parts[q][src : src + 32]

    return call(kernel, [((1024, 128), F32)], hi, lo, *blocks, *three)[0]


def to_y(parts):
    sent = [lax.ppermute(parts[q], "y", ring(4, q)) for q in range(1, 4)]
    return [parts[0]] + sent


def x_kernel(picks, refs, outs, sums):
    for m, (group, at) in enumerate(picks):
        rows = pl.ds(at * 128, 128)
        four = [r[rows, :] for r in refs[4 * group : 4 * group + 4]]
        sums[m] = (four[0] + four[1]) + (four[2] + four[3])
    x, zhi, zlo = lax.axis_index("x"), lax.axis_index("zhi"), lax.axis_index("zlo")
    for ahead in range(4):
        to = lax.rem(x + ahead, 4)
        xb, yh = to // 2, lax.rem(to, 2)
        for t in range(2):
            place = lax.rem(zhi + t, 2) * 2 + xb
            m = lax.rem(place - zlo + 4, 4)
            for h in range(2):
                at = t * 64 + h * 32
                outs[ahead][at : at + 32, :] = sums[
                    m, pl.ds(pl.multiple_of(h * 64 + yh * 32, 32), 32), :
                ]


def to_x(groups, picks):
    flat = [a for g in groups for a in g]
    n = len(flat)
    body = lambda *r: x_kernel(picks, r[:n], r[n : n + 4], r[n + 4])
    scratch = [pltpu.VMEM((4, 128, 128), F32)]
    outs = call(body, [((128, 128), F32)] * 4, *flat, scratch=scratch)
    return [outs[0]] + [lax.ppermute(outs[q], "x", ring(4, q)) for q in range(1, 4)]


def to_x_pair(even, odd, at):

    def kernel(*refs):
        sums, outs = refs[-1], refs[8:12]
        for parity, four, row in ((0, refs[:4], at), (1, refs[4:8], 0)):
            rows = pl.ds(row * 128, 128)
            v = [r[rows, :] for r in four]
            sums[parity] = (v[0] + v[1]) + (v[2] + v[3])
        x, zlo = lax.axis_index("x"), lax.axis_index("zlo")
        for ahead in range(4):
            to = lax.rem(x + ahead, 4)
            which, yh = lax.rem(to // 2 + zlo, 2), lax.rem(to, 2)
            for h in range(2):
                src = pl.ds(pl.multiple_of(h * 64 + yh * 32, 32), 32)
                outs[ahead][h * 32 : h * 32 + 32, :] = sums[which, src, :]

    scratch = [pltpu.VMEM((2, 128, 128), F32)]
    outs = call(kernel, [((64, 128), F32)] * 4, *even, *odd, scratch=scratch)
    return [outs[0]] + [lax.ppermute(outs[q], "x", ring(4, q)) for q in range(1, 4)]


def add_early(a, b, c, d, keep, send):
    v = (a[...] + b[...]) + (c[...] + d[...])
    keep[...] = v[:64]
    send[...] = v[64:]


def add_late(a, b, c, d, many, keep, send):
    early = (a[...] + b[...]) + (c[...] + d[...])
    v = [many[i * 64 : (i + 1) * 64, :] for i in range(16)]
    while len(v) > 1:
        v = [p + q for p, q in zip(v[::2], v[1::2])]
    x, zhi, zlo = lax.axis_index("x"), lax.axis_index("zhi"), lax.axis_index("zlo")
    ahead = jnp.where(lax.rem(x // 2 + zlo, 2) == 0, 2, 5)
    home = lax.rem(zlo + ahead, 4) // 2 == zhi
    keep[...] = jnp.where(home, early, v[0])
    send[...] = jnp.where(home, v[0], early)


def to_owner(kernel, *args):
    keep, send = call(kernel, [((64, 128), F32)] * 2, *args)
    return keep, lax.ppermute(send, "zhi", ring(2, 1))


def tile_kernel(keep_a, recv_a, keep_b, recv_b, ham, ovl):
    x, zhi, zlo = lax.axis_index("x"), lax.axis_index("zhi"), lax.axis_index("zlo")
    core = lax.axis_index("core")
    m = lax.rem(zhi * 2 + x // 2 - zlo + 4, 4)
    d = jnp.where(m < 2, m, m - 4)
    a0 = lax.rem(zhi * 4 + zlo + d + 8, 8) // 4
    for zi in range(2):
        parts = []
        for zj in range(2):
            far = lax.rem(zhi + zj, 2)
            late = lax.rem(zi + a0 + far, 2)
            kept = jnp.where(late == 0, keep_a[...], keep_b[...])
            came = jnp.where(late == 0, recv_a[...], recv_b[...])
            parts.append(jnp.where(far == 0, kept, came))
        for out, cut in ((ham, slice(0, 64)), (ovl, slice(64, 128))):
            v = jnp.concatenate([p[:, cut] for p in parts], axis=1)
            for h in range(2):
                c = lax.rem(core + h, 2)
                for k in range(4):
                    dst = pl.ds(pl.multiple_of(zi * 64 + k * 16 + c * 8, 8), 8)
                    out[dst, :] = v[h * 32 + k * 8 : h * 32 + k * 8 + 8, :]


def after(value, *others):
    return lax.optimization_barrier((value, *others))[0]


def body(orbitals, applied):
    core, swap = lax.axis_index("core"), ring(2, 1)
    orb = lax.all_to_all(orbitals, ("y", "x"), split_axis=1, concat_axis=0, tiled=True)
    by_parity = orb.reshape(2, 2, 32, K)
    mine = lax.dynamic_index_in_dim(by_parity, core, 1, False).reshape(64, K)
    theirs = lax.dynamic_index_in_dim(by_parity, 1 - core, 1, False).reshape(64, K)
    same = lax.ppermute(theirs, "core", swap)
    cross = lax.ppermute(mine, "core", swap)
    app = lax.all_to_all(after(applied, mine), ("y", "x"), split_axis=1, concat_axis=0, tiled=True)

    held = {(0, 0): mine, (0, 1): same}

    last = []

    def forward(d, h):
        ahead, behind = held[(d - 1, h)], held[((1 - d) % 8, h)]
        if d == 4:
            ahead, behind = ahead[:32], behind[32:]
        ahead = lax.ppermute(ahead, Z, z_ring(-1))
        behind = lax.ppermute(behind, Z, z_ring(1))
        if d == 4:
            last.extend((ahead, behind))
        else:
            held[(d, h)], held[(-d % 8, h)] = ahead, behind

    for d in range(1, 5):
        for h in range(2):
            forward(d, h)
    app_other = lax.ppermute(app, "core", swap)
    hi, lo = call(own_kernel, [((512, K), BF16)] * 2, orb, same, cross, app, app_other)
    blocks = lambda *ds: [held[(d % 8, h)] for d in ds for h in range(2)]
    y1 = to_y(products(hi, lo, blocks(0, 1, -1))[0])
    y2 = to_y(products(hi, lo, blocks(2, -2))[0])
    three, behind = products(hi, lo, blocks(3, -3), 2)
    y3 = to_y(behind)
    late = last_products(hi, lo, last, three)
    late = lax.all_to_all(late, ("y", "x"), split_axis=0, concat_axis=0, tiled=True)
    xa = to_x([y1, y2], [(0, 0), (0, 1), (1, 1), (0, 2)])
    xb = to_x_pair(y2, y3, 0)
    keep_a, recv_a = to_owner(add_early, *xa)
    keep_b, recv_b = to_owner(add_late, *xb, late)
    return call(tile_kernel, [((128, 128), F32)] * 2, keep_a, recv_a, keep_b, recv_b)


def solution(mesh):
    fine = Mesh(mesh.devices.reshape(4, 4, 2, 4, 2), AXES)
    placed = P(AXES, None)
    out = P(("zhi", "x", "core"), ("zlo", "y"))

    return jax.shard_map(
        body, mesh=fine, in_specs=(placed, placed), out_specs=(out, out), check_vma=False
    )
```

```python
import jax
import jax.numpy as jnp
from jax import lax
from jax.experimental import pallas as pl
from jax.experimental.pallas import tpu as pltpu
from jax.sharding import Mesh, PartitionSpec as P


AXES = ("zlo", "y", "zhi", "x", "core")
Z = ("zlo", "zhi")
F32, BF16 = jnp.float32, jnp.bfloat16
K = 1792
NT = (((1,), (1,)), ((), ()))
VMEM = pl.BlockSpec(memory_space=pltpu.VMEM)


def z_ring(step):
    place = lambda z: (z % 4) * 2 + z // 4
    return [(place(z), place((z + step) % 8)) for z in range(8)]


def ring(n, step):
    return [(i, (i + step) % n) for i in range(n)]


def call(kernel, shapes, *args, scratch=()):
    out = [jax.ShapeDtypeStruct(s, t) for s, t in shapes]
    return pl.pallas_call(
        kernel,
        out_shape=out,
        in_specs=[VMEM] * len(args),
        out_specs=[VMEM] * len(out),
        scratch_shapes=list(scratch),
        compiler_params=pltpu.CompilerParams(vmem_limit_bytes=20 * 2**20),
    )(*args)


def own_kernel(orb, same, cross, app, app_other, hi, lo):
    y, core = lax.axis_index("y"), lax.axis_index("core")
    first = core == 0

    def step(t, carry):
        ahead, x = t // 4, lax.rem(t, 4)
        to = lax.rem(y + ahead, 4)
        src = pl.ds(pl.multiple_of(to * 32 + x * 8, 8), 8)
        part = pl.ds(pl.multiple_of((to // 2) * 32 + x * 8, 8), 8)
        theirs = jnp.where(lax.rem(to, 2) == core, same[part, :], cross[part, :])
        for h, (a, b) in enumerate(((app[src, :], app_other[src, :]), (orb[src, :], theirs))):
            v = jnp.concatenate([jnp.where(first, a, b), jnp.where(first, b, a)], 0)
            top = v.astype(BF16)
            dst = pl.ds(pl.multiple_of(ahead * 128 + h * 64 + x * 16, 16), 16)
            hi[dst, :] = top
            lo[dst, :] = (v - top.astype(F32)).astype(BF16)
        return carry

    lax.fori_loop(0, 16, step, 0)


def product(blocks, hi, lo):
    v = jnp.concatenate([b[...] for b in blocks], 0)
    top = v.astype(BF16)
    low = (v - top.astype(F32)).astype(BF16)
    both = jnp.concatenate([top, low], 0)
    rows, parts = v.shape[0], []
    for half in range(2):
        cols = slice(half * 256, (half + 1) * 256)
        p = lax.dot_general(both, hi[cols, :], NT, preferred_element_type=F32)
        r = lax.dot_general(top, lo[cols, :], NT, preferred_element_type=F32)
        total = (p[:rows] + p[rows:]) + r
        parts += [total[:, :128], total[:, 128:]]
    return parts


def products(hi, lo, blocks, groups=1):
    rows = sum(b.shape[0] for b in blocks) // groups

    def kernel(hi, lo, *refs):
        n = len(blocks)
        for q, part in enumerate(product(refs[:n], hi, lo)):
            for g in range(groups):
                refs[n + 4 * g + q][...] = part[g * rows : (g + 1) * rows]

    outs = call(kernel, [((rows, 128), F32)] * (4 * groups), hi, lo, *blocks)
    return [outs[4 * g : 4 * g + 4] for g in range(groups)]


def last_products(hi, lo, blocks, three):

    def kernel(hi, lo, *refs):
        n = len(blocks)
        out = refs[-1]
        y, zlo = lax.axis_index("y"), lax.axis_index("zlo")
        four = product(refs[:n], hi, lo)
        for d, parts in ((3, [r[...] for r in refs[n : n + 4]]), (4, four)):
            xb = lax.rem(zlo + d, 2)
            for q in range(4):
                to = lax.rem(y + q, 4) * 4 + xb * 2
                for yh in range(2):
                    for h in range(2):
                        at = pl.multiple_of((to + yh) * 64 + h * 32, 32)
                        src = h * 64 + yh * 32
                        out[pl.ds(at, 32), :] = parts[q][src : src + 32]

    return call(kernel, [((1024, 128), F32)], hi, lo, *blocks, *three)[0]


def to_y(parts):
    sent = [lax.ppermute(parts[q], "y", ring(4, q)) for q in range(1, 4)]
    return [parts[0]] + sent


def x_kernel(picks, refs, outs, sums):
    for m, (group, at) in enumerate(picks):
        rows = pl.ds(at * 128, 128)
        four = [r[rows, :] for r in refs[4 * group : 4 * group + 4]]
        sums[m] = (four[0] + four[1]) + (four[2] + four[3])
    x, zhi, zlo = lax.axis_index("x"), lax.axis_index("zhi"), lax.axis_index("zlo")
    for ahead in range(4):
        to = lax.rem(x + ahead, 4)
        xb, yh = to // 2, lax.rem(to, 2)
        for t in range(2):
            place = lax.rem(zhi + t, 2) * 2 + xb
            m = lax.rem(place - zlo + 4, 4)
            for h in range(2):
                at = t * 64 + h * 32
                outs[ahead][at : at + 32, :] = sums[
                    m, pl.ds(pl.multiple_of(h * 64 + yh * 32, 32), 32), :
                ]


def to_x(groups, picks):
    flat = [a for g in groups for a in g]
    n = len(flat)
    body = lambda *r: x_kernel(picks, r[:n], r[n : n + 4], r[n + 4])
    scratch = [pltpu.VMEM((4, 128, 128), F32)]
    outs = call(body, [((128, 128), F32)] * 4, *flat, scratch=scratch)
    return [outs[0]] + [lax.ppermute(outs[q], "x", ring(4, q)) for q in range(1, 4)]


def to_x_pair(even, odd, at):

    def kernel(*refs):
        sums, outs = refs[-1], refs[8:12]
        for parity, four, row in ((0, refs[:4], at), (1, refs[4:8], 0)):
            rows = pl.ds(row * 128, 128)
            v = [r[rows, :] for r in four]
            sums[parity] = (v[0] + v[1]) + (v[2] + v[3])
        x, zlo = lax.axis_index("x"), lax.axis_index("zlo")
        for ahead in range(4):
            to = lax.rem(x + ahead, 4)
            which, yh = lax.rem(to // 2 + zlo, 2), lax.rem(to, 2)
            for h in range(2):
                src = pl.ds(pl.multiple_of(h * 64 + yh * 32, 32), 32)
                outs[ahead][h * 32 : h * 32 + 32, :] = sums[which, src, :]

    scratch = [pltpu.VMEM((2, 128, 128), F32)]
    outs = call(kernel, [((64, 128), F32)] * 4, *even, *odd, scratch=scratch)
    return [outs[0]] + [lax.ppermute(outs[q], "x", ring(4, q)) for q in range(1, 4)]


def add_early(a, b, c, d, keep, send):
    v = (a[...] + b[...]) + (c[...] + d[...])
    keep[...] = v[:64]
    send[...] = v[64:]


def add_late(a, b, c, d, many, keep, send):
    early = (a[...] + b[...]) + (c[...] + d[...])
    v = [many[i * 64 : (i + 1) * 64, :] for i in range(16)]
    while len(v) > 1:
        v = [p + q for p, q in zip(v[::2], v[1::2])]
    x, zhi, zlo = lax.axis_index("x"), lax.axis_index("zhi"), lax.axis_index("zlo")
    ahead = jnp.where(lax.rem(x // 2 + zlo, 2) == 0, 2, 5)
    home = lax.rem(zlo + ahead, 4) // 2 == zhi
    keep[...] = jnp.where(home, early, v[0])
    send[...] = jnp.where(home, v[0], early)


def to_owner(kernel, *args):
    keep, send = call(kernel, [((64, 128), F32)] * 2, *args)
    return keep, lax.ppermute(send, "zhi", ring(2, 1))


def tile_kernel(keep_a, recv_a, keep_b, recv_b, ham, ovl):
    x, zhi, zlo = lax.axis_index("x"), lax.axis_index("zhi"), lax.axis_index("zlo")
    core = lax.axis_index("core")
    m = lax.rem(zhi * 2 + x // 2 - zlo + 4, 4)
    d = jnp.where(m < 2, m, m - 4)
    a0 = lax.rem(zhi * 4 + zlo + d + 8, 8) // 4
    for zi in range(2):
        parts = []
        for zj in range(2):
            far = lax.rem(zhi + zj, 2)
            late = lax.rem(zi + a0 + far, 2)
            kept = jnp.where(late == 0, keep_a[...], keep_b[...])
            came = jnp.where(late == 0, recv_a[...], recv_b[...])
            parts.append(jnp.where(far == 0, kept, came))
        for out, cut in ((ham, slice(0, 64)), (ovl, slice(64, 128))):
            v = jnp.concatenate([p[:, cut] for p in parts], axis=1)
            for h in range(2):
                c = lax.rem(core + h, 2)
                for k in range(4):
                    dst = pl.ds(pl.multiple_of(zi * 64 + k * 16 + c * 8, 8), 8)
                    out[dst, :] = v[h * 32 + k * 8 : h * 32 + k * 8 + 8, :]


def after(value, *others):
    return lax.optimization_barrier((value, *others))[0]


def body(orbitals, applied):
    core, swap = lax.axis_index("core"), ring(2, 1)
    orb = lax.all_to_all(orbitals, ("y", "x"), split_axis=1, concat_axis=0, tiled=True)
    by_parity = orb.reshape(2, 2, 32, K)
    mine = lax.dynamic_index_in_dim(by_parity, core, 1, False).reshape(64, K)
    rest = after(by_parity, mine)
    theirs = lax.dynamic_index_in_dim(rest, 1 - core, 1, False).reshape(64, K)
    same = lax.ppermute(theirs, "core", swap)
    cross = lax.ppermute(mine, "core", swap)
    app = lax.all_to_all(after(applied, mine), ("y", "x"), split_axis=1, concat_axis=0, tiled=True)

    held = {(0, 0): mine, (0, 1): same}

    last, cuts = [], []

    def forward(d, h):
        ahead, behind = held[(d - 1, h)], held[((1 - d) % 8, h)]
        if d == 4:
            ahead, behind = ahead[:32], behind[32:]
            cuts.extend((ahead, behind))
        ahead = lax.ppermute(ahead, Z, z_ring(-1))
        behind = lax.ppermute(behind, Z, z_ring(1))
        if d == 4:
            last.extend((ahead, behind))
        else:
            held[(d, h)], held[(-d % 8, h)] = ahead, behind

    for d in range(1, 5):
        for h in range(2):
            forward(d, h)
    app_other = lax.ppermute(app, "core", swap)
    hi, lo = call(own_kernel, [((512, K), BF16)] * 2, orb, same, cross, app, app_other)
    blocks = lambda *ds: [held[(d % 8, h)] for d in ds for h in range(2)]
    y1 = to_y(products(hi, lo, blocks(0, 1, -1))[0])
    y2 = to_y(products(hi, lo, blocks(2, -2))[0])
    three, behind = products(hi, lo, blocks(3, -3), 2)
    y3 = to_y(behind)
    late = last_products(hi, lo, last, three)
    late = lax.all_to_all(late, ("y", "x"), split_axis=0, concat_axis=0, tiled=True)
    y1[0] = after(y1[0], *cuts[:2])
    xa = to_x([y1, y2], [(0, 0), (0, 1), (1, 1), (0, 2)])
    xb = to_x_pair(y2, y3, 0)
    keep_a, recv_a = to_owner(add_early, *xa)
    keep_b, recv_b = to_owner(add_late, *xb, late)
    return call(tile_kernel, [((128, 128), F32)] * 2, keep_a, recv_a, keep_b, recv_b)


def solution(mesh):
    fine = Mesh(mesh.devices.reshape(4, 4, 2, 4, 2), AXES)
    placed = P(AXES, None)
    out = P(("zhi", "x", "core"), ("zlo", "y"))

    return jax.shard_map(
        body, mesh=fine, in_specs=(placed, placed), out_specs=(out, out), check_vma=False
    )
```

```python
import jax
import jax.numpy as jnp
from jax import lax
from jax.experimental import pallas as pl
from jax.experimental.pallas import tpu as pltpu
from jax.sharding import Mesh, PartitionSpec as P


AXES = ("zlo", "y", "zhi", "x", "core")
Z = ("zlo", "zhi")
F32, BF16 = jnp.float32, jnp.bfloat16
K = 1792
NT = (((1,), (1,)), ((), ()))
VMEM = pl.BlockSpec(memory_space=pltpu.VMEM)


def z_ring(step):
    place = lambda z: (z % 4) * 2 + z // 4
    return [(place(z), place((z + step) % 8)) for z in range(8)]


def ring(n, step):
    return [(i, (i + step) % n) for i in range(n)]


def call(kernel, shapes, *args, scratch=()):
    out = [jax.ShapeDtypeStruct(s, t) for s, t in shapes]
    return pl.pallas_call(
        kernel,
        out_shape=out,
        in_specs=[VMEM] * len(args),
        out_specs=[VMEM] * len(out),
        scratch_shapes=list(scratch),
        compiler_params=pltpu.CompilerParams(vmem_limit_bytes=20 * 2**20),
    )(*args)


def own_kernel(orb, same, cross, app, app_other, hi, lo):
    y, core = lax.axis_index("y"), lax.axis_index("core")
    first = core == 0

    def step(t, carry):
        ahead, x = t // 4, lax.rem(t, 4)
        to = lax.rem(y + ahead, 4)
        src = pl.ds(pl.multiple_of(to * 32 + x * 8, 8), 8)
        part = pl.ds(pl.multiple_of((to // 2) * 32 + x * 8, 8), 8)
        theirs = jnp.where(lax.rem(to, 2) == core, same[part, :], cross[part, :])
        for h, (a, b) in enumerate(((app[src, :], app_other[src, :]), (orb[src, :], theirs))):
            v = jnp.concatenate([jnp.where(first, a, b), jnp.where(first, b, a)], 0)
            top = v.astype(BF16)
            dst = pl.ds(pl.multiple_of(ahead * 128 + h * 64 + x * 16, 16), 16)
            hi[dst, :] = top
            lo[dst, :] = (v - top.astype(F32)).astype(BF16)
        return carry

    lax.fori_loop(0, 16, step, 0)


def product(blocks, hi, lo):
    v = jnp.concatenate([b[...] for b in blocks], 0)
    top = v.astype(BF16)
    low = (v - top.astype(F32)).astype(BF16)
    both = jnp.concatenate([top, low], 0)
    rows, parts = v.shape[0], []
    for half in range(2):
        cols = slice(half * 256, (half + 1) * 256)
        p = lax.dot_general(both, hi[cols, :], NT, preferred_element_type=F32)
        r = lax.dot_general(top, lo[cols, :], NT, preferred_element_type=F32)
        total = (p[:rows] + p[rows:]) + r
        parts += [total[:, :128], total[:, 128:]]
    return parts


def products(hi, lo, blocks, groups=1):
    rows = sum(b.shape[0] for b in blocks) // groups

    def kernel(hi, lo, *refs):
        n = len(blocks)
        for q, part in enumerate(product(refs[:n], hi, lo)):
            for g in range(groups):
                refs[n + 4 * g + q][...] = part[g * rows : (g + 1) * rows]

    outs = call(kernel, [((rows, 128), F32)] * (4 * groups), hi, lo, *blocks)
    return [outs[4 * g : 4 * g + 4] for g in range(groups)]


def to_y(parts):
    sent = [lax.ppermute(parts[q], "y", ring(4, q)) for q in range(1, 4)]
    return [parts[0]] + sent


def x_kernel(picks, refs, outs, sums):
    for m, (group, at) in enumerate(picks):
        rows = pl.ds(at * 128, 128)
        four = [r[rows, :] for r in refs[4 * group : 4 * group + 4]]
        sums[m] = (four[0] + four[1]) + (four[2] + four[3])
    x, zhi, zlo = lax.axis_index("x"), lax.axis_index("zhi"), lax.axis_index("zlo")
    for ahead in range(4):
        to = lax.rem(x + ahead, 4)
        xb, yh = to // 2, lax.rem(to, 2)
        for t in range(2):
            place = lax.rem(zhi + t, 2) * 2 + xb
            m = lax.rem(place - zlo + 4, 4)
            for h in range(2):
                at = t * 64 + h * 32
                outs[ahead][at : at + 32, :] = sums[
                    m, pl.ds(pl.multiple_of(h * 64 + yh * 32, 32), 32), :
                ]


def to_x(groups, picks):
    flat = [a for g in groups for a in g]
    n = len(flat)
    body = lambda *r: x_kernel(picks, r[:n], r[n : n + 4], r[n + 4])
    scratch = [pltpu.VMEM((4, 128, 128), F32)]
    outs = call(body, [((128, 128), F32)] * 4, *flat, scratch=scratch)
    got = [outs[0]] + [lax.ppermute(outs[q], "x", ring(4, q)) for q in range(1, 4)]

    def add(a, b, c, d, keep, send):
        v = (a[...] + b[...]) + (c[...] + d[...])
        keep[...] = v[:64]
        send[...] = v[64:]

    keep, send = call(add, [((64, 128), F32)] * 2, *got)
    return keep, lax.ppermute(send, "zhi", ring(2, 1))


def tile_kernel(keep_a, recv_a, keep_b, recv_b, ham, ovl):
    x, zhi, zlo = lax.axis_index("x"), lax.axis_index("zhi"), lax.axis_index("zlo")
    core = lax.axis_index("core")
    m = lax.rem(zhi * 2 + x // 2 - zlo + 4, 4)
    d = jnp.where(m < 2, m, m - 4)
    a0 = lax.rem(zhi * 4 + zlo + d + 8, 8) // 4
    for zi in range(2):
        parts = []
        for zj in range(2):
            far = lax.rem(zhi + zj, 2)
            late = lax.rem(zi + a0 + far, 2)
            kept = jnp.where(late == 0, keep_a[...], keep_b[...])
            came = jnp.where(late == 0, recv_a[...], recv_b[...])
            parts.append(jnp.where(far == 0, kept, came))
        for out, cut in ((ham, slice(0, 64)), (ovl, slice(64, 128))):
            v = jnp.concatenate([p[:, cut] for p in parts], axis=1)
            for h in range(2):
                c = lax.rem(core + h, 2)
                for k in range(4):
                    dst = pl.ds(pl.multiple_of(zi * 64 + k * 16 + c * 8, 8), 8)
                    out[dst, :] = v[h * 32 + k * 8 : h * 32 + k * 8 + 8, :]


def after(value, *others):
    return lax.optimization_barrier((value, *others))[0]


def body(orbitals, applied):
    core, swap = lax.axis_index("core"), ring(2, 1)
    orb = lax.all_to_all(orbitals, ("y", "x"), split_axis=1, concat_axis=0, tiled=True)
    by_parity = orb.reshape(2, 2, 32, K)
    mine = lax.dynamic_index_in_dim(by_parity, core, 1, False).reshape(64, K)
    rest = after(by_parity, mine)
    theirs = lax.dynamic_index_in_dim(rest, 1 - core, 1, False).reshape(64, K)
    same = lax.ppermute(theirs, "core", swap)
    cross = lax.ppermute(mine, "core", swap)
    app = lax.all_to_all(after(applied, mine), ("y", "x"), split_axis=1, concat_axis=0, tiled=True)

    held = {(0, 0): mine, (0, 1): same}

    last, cuts = [], []

    def forward(d, h):
        ahead, behind = held[(d - 1, h)], held[((1 - d) % 8, h)]
        if d == 4:
            ahead, behind = ahead[:32], behind[32:]
            cuts.extend((ahead, behind))
        ahead = lax.ppermute(ahead, Z, z_ring(-1))
        behind = lax.ppermute(behind, Z, z_ring(1))
        if d == 4:
            last.extend((ahead, behind))
        else:
            held[(d, h)], held[(-d % 8, h)] = ahead, behind

    for d in range(1, 5):
        for h in range(2):
            forward(d, h)
    app_other = lax.ppermute(app, "core", swap)
    hi, lo = call(own_kernel, [((512, K), BF16)] * 2, orb, same, cross, app, app_other)
    blocks = lambda *ds: [held[(d % 8, h)] for d in ds for h in range(2)]
    y1 = to_y(products(hi, lo, blocks(0, 1, -1))[0])
    y2 = to_y(products(hi, lo, blocks(2, -2))[0])
    y3 = to_y(products(hi, lo, blocks(3, -3))[0])
    y4 = to_y(products(hi, lo, last)[0])
    y1[0] = after(y1[0], *cuts[:2])
    keep_a, recv_a = to_x([y1, y2], [(0, 0), (0, 1), (1, 1), (0, 2)])
    keep_b, recv_b = to_x([y2, y3, y4], [(2, 0), (1, 1), (0, 0), (1, 0)])
    return call(tile_kernel, [((128, 128), F32)] * 2, keep_a, recv_a, keep_b, recv_b)


def solution(mesh):
    fine = Mesh(mesh.devices.reshape(4, 4, 2, 4, 2), AXES)
    placed = P(AXES, None)
    out = P(("zhi", "x", "core"), ("zlo", "y"))

    return jax.shard_map(
        body, mesh=fine, in_specs=(placed, placed), out_specs=(out, out), check_vma=False
    )
```
